32 devices in a mesh: tile: 4 (over x, core), chan: 4 (over z), beam: 2 (over y).
Axes of the slice: x: 2, y: 2, z: 4, core: 2. Of those that a mesh axis runs over, the one named last changes fastest.
Arguments:
- voltages: bfloat16 [32, 128, 2, 2, 1536], P(None, 'tile', None, None, 'chan'), may hold values from -6 to 6
- calib_gain: float32 [128, 2, 2, 1536], P(('tile', 'beam'), None, None, 'chan'), may hold values from -0.375 to 0.375
- tile_flags: int32 [128], P(('tile', 'beam')), may hold values 0 or 1
- delays: float32 [64, 128], P(None, 'tile'), may hold values from -4 to 4
- pointing: int32 [2], P('beam'), may hold values from 0 to 63
- synth_filter: float32 [12, 128], replicated, may hold values from -0.5 to 0.5
Outputs:
- streams: float32 [32, 2, 2, 12, 256], P('tile', 'beam', None, 'chan')
The draws below stay inside these ranges and needn't reach their ends.
Inputs may be any that keep to these rules, and one draw needn't show every extreme that they name: `tile_flags`: 1 marks a tile in use. `pointing`: a row of delays, one of 64.
All inputs are finite; a program needn't handle non-finite values. No bound on the sum of `tile_flags` on one device may be relied on, other than what follows from the above.
Results may differ from the reference program's by a relative error of at most 0.0003.
Values sent between devices are 32-bit elements; how exact they have to be, the bound alone decides.
A program may use at most 64 MiB of HBM per device.

```python
import math
import jax
import jax.numpy as jnp
from jax import lax

NT = 128
K = 128
COARSE = 12
TAPS = 12
NPOINT = 64
T_SIZE = 32
BEAMS = 2
CHANS = 1536


def touch_ends(result, rng, low, top_value):
    spot = [jax.random.randint(jax.random.fold_in(rng, axis), (), 0, length) for axis, length in enumerate(result.shape)]
    widest = result.shape.index(max(result.shape))
    beside = spot[:widest] + [(spot[widest] + 1) % result.shape[widest]] + spot[widest + 1:]
    return result.at[tuple(spot)].set(low).at[tuple(beside)].set(top_value)


def spiked(entries, rng, source, target, blocks, factor):
    owner, partner = [(jnp.arange(entries.shape[axis_at]) // (entries.shape[axis_at] // blocks)).reshape([-1 if axis == axis_at else 1 for axis in range(entries.ndim)]) for axis_at in (source, target)]
    chosen = jax.random.permutation(rng, blocks)[partner]
    strong = (owner == chosen) | (owner == (partner + blocks // 2) % blocks)
    return jnp.where(strong, factor * entries, entries)


def block_scale(stream_key, extent, pieces, low, top_value):
    def one(dim, parts):
        steps = jax.random.uniform(jax.random.fold_in(jax.random.fold_in(stream_key, 6), dim), (parts,), jnp.float32, low / len(pieces), top_value / len(pieces))
        return jnp.repeat(jnp.exp(steps), extent[dim] // parts).reshape((-1,) + (1,) * (len(extent) - dim - 1))

    level = one(*pieces[0])
    for cut in pieces[1:]:
        level = level * one(*cut)
    return level


def noise(key, dims, deviation, limit, shards=(), kind=jnp.bfloat16):
    drawn = deviation * jax.random.normal(key, dims, jnp.float32)
    if shards:
        drawn = drawn * block_scale(key, dims, shards, -0.22, 0.18)
    return jnp.clip(drawn, -limit, limit).astype(kind)


def gaussian_with(own_key, dims, deviation, reach, split, heavy, kind=jnp.bfloat16):
    values = deviation * jax.random.normal(own_key, dims, jnp.float32)
    if split:
        values = values * block_scale(own_key, dims, split, -0.22, 0.18)
    return jnp.clip(spiked(values, jax.random.fold_in(own_key, 3), *heavy), -reach, reach).astype(kind)


def setup_inputs(seed: int = 0) -> dict:
    key_of = jax.random.split(jax.random.key(seed), 7)
    voltages = gaussian_with(key_of[0], (T_SIZE, NT, 2, 2, CHANS), 1.0, 6.0, ((1, 4), (4, 4)), (1, 0, 4, 2.0))
    calib_gain = noise(key_of[1], (NT, 2, 2, CHANS), (0.7 * NT ** -0.5), 0.375, ((0, 8), (3, 4)), jnp.float32)
    tile_flags = touch_ends((jax.random.randint(key_of[2], (NT,), 0, 4) < 3).astype(jnp.int32), jax.random.fold_in(key_of[2], 1), 0, 1)
    delays = jnp.clip(jax.random.uniform(key_of[3], (NPOINT, NT), jnp.float32, -4.0, 4.0) * block_scale(key_of[3], (NPOINT, NT), ((1, 4),), -0.4, 0.0), -4.0, 4.0)
    pointing = jax.random.randint(key_of[4], (BEAMS,), 0, NPOINT).astype(jnp.int32)
    synth_filter = jnp.clip(jax.random.uniform(key_of[5], (TAPS, K), jnp.float32, -0.5, 0.5), -0.5, 0.5)
    return {"voltages": voltages, "calib_gain": calib_gain, "tile_flags": tile_flags, "delays": delays, "pointing": pointing, "synth_filter": synth_filter}


TWO_PI = 6.283185307179586

def channel_frequency(first_index, length):
    global_idx = first_index + jnp.arange(length, dtype=jnp.int32)
    physical = global_idx % COARSE * K + global_idx // COARSE
    return (physical.astype(jnp.float32) + 0.5) / (K * COARSE)

def beam_weights(calib_gain, tile_flags, tile_delay, frequency):
    phase_angle = (TWO_PI * tile_delay)[:, :, None] * frequency[None, None, :]
    cosine = jnp.cos(phase_angle)[:, :, None, :]
    sine_part = jnp.sin(phase_angle)[:, :, None, :]
    gain_re = calib_gain[:, :, 0, :][None]
    gain_im = calib_gain[:, :, 1, :][None]
    in_use = tile_flags.astype(jnp.float32)[None, :, None, None]
    weight_re = in_use * (gain_re * cosine + gain_im * sine_part)
    weight_im = in_use * (gain_im * cosine - gain_re * sine_part)
    return (weight_re, weight_im)

def reference(voltages, calib_gain, tile_flags, delays, pointing, synth_filter):
    tile_delay = delays[pointing]
    frequency = channel_frequency(0, K * COARSE)
    weight_re, weight_im = beam_weights(calib_gain, tile_flags, tile_delay, frequency)
    row_count = voltages.shape[0]
    beams = pointing.shape[0]
    chans = voltages.shape[-1]

    def accumulate(carried, items):
        volt, tile_re, tile_im = items
        volt = volt.astype(jnp.float32)
        volt_re = volt[:, None, :, 0, :]
        volt_im = volt[:, None, :, 1, :]
        beam_re = carried[0] + (tile_re[None] * volt_re - tile_im[None] * volt_im)
        beam_im = carried[1] + (tile_re[None] * volt_im + tile_im[None] * volt_re)
        return ((beam_re, beam_im), None)
    zeros = jnp.zeros((row_count, beams, 2, chans), jnp.float32)
    (beam_re, beam_im), unused = lax.scan(accumulate, (zeros, zeros), (jnp.moveaxis(voltages, 1, 0), jnp.moveaxis(weight_re, 1, 0), jnp.moveaxis(weight_im, 1, 0)))
    grid_shape = (row_count, beams, 2, K, COARSE)
    combined = lax.complex(beam_re, beam_im).reshape(grid_shape)
    spectra = jnp.fft.ifft(combined, axis=3) * math.sqrt(K)
    spectra = jnp.moveaxis(spectra, 3, 4)
    padded = jnp.pad(spectra, ((TAPS - 1, 0), (0, 0), (0, 0), (0, 0), (0, 0)))
    streams = jnp.zeros_like(spectra)
    for offset in range(TAPS):
        begin = TAPS - 1 - offset
        streams = streams + synth_filter[offset] * padded[begin:begin + row_count]
    return jnp.concatenate([jnp.real(streams), jnp.imag(streams)], axis=-1)
```

```python
import functools
import math

import jax
import jax.numpy as jnp
import numpy as np
from jax import lax
from jax.experimental import pallas as pl
from jax.experimental.pallas import tpu as pltpu
from jax.sharding import PartitionSpec as P

COARSE = 12
LANES = 128
MESH = pl.DeviceIdType.MESH
F32 = jnp.float32
BF16 = jnp.bfloat16


def even_fit(func, degree):
    series = np.polynomial.chebyshev.Chebyshev.interpolate(
        lambda u: func(np.sqrt(u)), degree, domain=[0.0, 0.25]
    )
    return [float(v) for v in series.convert(kind=np.polynomial.Polynomial).coef]


COS_COEF = even_fit(lambda r: np.cos(2 * np.pi * r), 7)
SIN_COEF = even_fit(lambda r: 2 * np.pi * np.sinc(2 * r), 7)


def horner(coef, u):
    total = jnp.full_like(u, coef[-1])
    for value in coef[-2::-1]:
        total = total * u + value
    return total


def split_bf16(table):
    high = table.astype(BF16)
    low = (table - high.astype(np.float64)).astype(BF16)
    return high, low


def dft_table(nz, fz):
    k = nz * fz
    f = np.arange(k)
    m = np.arange(k)
    angle = 2 * np.pi * (f[:, None] * m[None, :] % k) / k
    cosine, sine = np.cos(angle) / math.sqrt(k), np.sin(angle) / math.sqrt(k)
    out = np.zeros((nz, 2, 2, fz, 2, 2, k))
    for p in range(2):
        out[:, p, 0, :, p, 0] = cosine.reshape(nz, fz, k)
        out[:, p, 0, :, p, 1] = sine.reshape(nz, fz, k)
        out[:, p, 1, :, p, 0] = -sine.reshape(nz, fz, k)
        out[:, p, 1, :, p, 1] = cosine.reshape(nz, fz, k)
    return split_bf16(out.reshape(nz * 4 * fz, 4 * k))


def gather_table(nz, fz, cz):
    width = fz * COARSE
    out = np.zeros((width, width), np.float64)
    for c in range(cz):
        for z in range(nz):
            for f in range(fz):
                out[f * COARSE + z * cz + c, (c * nz + z) * fz + f] = 1.0
    return out.astype(BF16)


def kernel(
    cfg,
    volt_ref,
    gain_ref,
    flag_ref,
    delay_ref,
    point_ref,
    synth_ref,
    chan_ref,
    perm_ref,
    dfth_ref,
    dftl_ref,
    out_ref,
    volt,
    gains,
    w_re,
    w_im,
    acc,
    part,
    recv,
    packed,
    inbox,
    spec,
    dft_h,
    dft_l,
    volt_sem,
    table_sem,
    gain_send,
    gain_recv,
    part_send,
    part_recv,
    pack_send,
    pack_recv,
):
    nt, nz, nb, tb, n_all, taps, fz, cz, halo, exchange = cfg
    tile = lax.axis_index("tile")
    chan = lax.axis_index("chan")
    beam = lax.axis_index("beam")
    rows_t = n_all * 4 * cz
    rows_n = 4 * cz

    def peer(t, z, b):
        return {"tile": t, "chan": z, "beam": b}

    order = sorted(range(1, nt), key=lambda d: abs(2 * d - nt)) + [0]
    loads = []
    for slot, d in enumerate(order):
        block = lax.rem(tile + d, nt)
        loads.append(
            pltpu.make_async_copy(
                volt_ref.at[pl.ds(pl.multiple_of(block * (tb * rows_t), 16), tb * rows_t)],
                volt.at[slot],
                volt_sem.at[slot],
            )
        )
    loads[0].start()

    barrier = pltpu.get_barrier_semaphore()
    count = 0
    for dt in range(nt):
        for dz in range(nz):
            if dt or dz:
                pl.semaphore_signal(
                    barrier,
                    inc=1,
                    device_id=peer(lax.rem(tile + dt, nt), lax.rem(chan + dz, nz), beam),
                    device_id_type=MESH,
                )
                count += 1
    for db in range(1, nb):
        pl.semaphore_signal(
            barrier, inc=1, device_id=peer(tile, chan, lax.rem(beam + db, nb)), device_id_type=MESH
        )
        count += 1

    for load in loads[1:]:
        load.start()
    tables = [
        pltpu.make_async_copy(dfth_ref, dft_h, table_sem.at[0]),
        pltpu.make_async_copy(dftl_ref, dft_l, table_sem.at[1]),
    ]
    for copy in tables:
        copy.start()

    pair = 2 * rows_n
    row = lax.broadcasted_iota(jnp.int32, (pair, LANES), 0)
    first = row < rows_n
    even = lax.rem(row, 2) == 0
    n_own = n_all // nb

    if exchange:
        for i in range(n_own // 2):
            use = jnp.where(
                first, flag_ref[2 * i].astype(F32), flag_ref[2 * i + 1].astype(F32)
            )
            gains[beam, pl.ds(i * pair, pair), :] = use * gain_ref[pl.ds(i * pair, pair), :]

    for h in range(1, halo + 1):

        @pl.when(tile < h)
        def _():
            inbox[h] = jnp.zeros(inbox.shape[1:], F32)

    pl.semaphore_wait(barrier, count)

    gain_copies = []
    if exchange:
        for db in range(1, nb):
            copy = pltpu.make_async_remote_copy(
                src_ref=gains.at[beam],
                dst_ref=gains.at[beam],
                send_sem=gain_send.at[db - 1],
                recv_sem=gain_recv.at[db - 1],
                device_id=peer(tile, chan, lax.rem(beam + db, nb)),
                device_id_type=MESH,
            )
            copy.start()
            gain_copies.append(copy)

    select = lax.broadcasted_iota(jnp.int32, delay_ref.shape, 1) == point_ref[0]
    delay = jnp.sum(jnp.where(select, delay_ref[...], 0.0), axis=1, keepdims=True)
    delay = jnp.broadcast_to(delay, (n_all, LANES))
    frequency = (chan_ref[...] + (chan * fz).astype(F32) + 0.5) / (COARSE * nz * fz)

    def phase(i):
        cycles = (
            jnp.where(
                first,
                jnp.broadcast_to(delay[2 * i : 2 * i + 1], (pair, LANES)),
                jnp.broadcast_to(delay[2 * i + 1 : 2 * i + 2], (pair, LANES)),
            )
            * frequency
        )
        turn = cycles - jnp.floor(cycles + 0.5)
        square = turn * turn
        return horner(COS_COEF, square), turn * horner(SIN_COEF, square)

    for i in range(n_all // 2):
        cosine, sine = phase(i)
        w_re[pl.ds(i * pair, pair), :] = cosine
        w_im[pl.ds(i * pair, pair), :] = sine

    for copy in gain_copies:
        copy.wait_recv()

    for i in range(n_all // 2):
        if exchange:
            owner, inner = divmod(2 * i, n_own)
            gain = gains[owner, pl.ds(inner * rows_n, pair), :]
        else:
            gain = gain_ref[pl.ds(i * pair, pair), :]
        cosine = w_re[pl.ds(i * pair, pair), :]
        sine = w_im[pl.ds(i * pair, pair), :]
        swapped = jnp.where(
            even, pltpu.roll(gain, pair - 1, 0), -pltpu.roll(gain, 1, 0)
        )
        weight = gain * cosine + swapped * sine
        w_re[pl.ds(i * pair, pair), :] = jnp.where(even, weight, pltpu.roll(weight, 1, 0))
        w_im[pl.ds(i * pair, pair), :] = jnp.where(even, pltpu.roll(weight, pair - 1, 0), weight)

    quad = 2 * pair
    unroll = 2
    part_copies = []
    for slot, d in enumerate(order):
        loads[slot].wait()

        def step(s, carry):
            sums = [[jnp.zeros((quad, LANES), F32)] * 2 for _ in range(unroll)]
            for q in range(n_all // 4):
                wr = w_re[pl.ds(q * quad, quad), :]
                wi = w_im[pl.ds(q * quad, quad), :]
                for u in range(unroll):
                    begin = pl.multiple_of((s * unroll + u) * rows_t, 16) + q * quad
                    v = volt[slot, pl.ds(begin, quad), :].astype(F32)
                    sums[u] = [sums[u][0] + wr * v, sums[u][1] + wi * v]
            for u in range(unroll):
                begin = pl.multiple_of((s * unroll + u) * quad, 8)
                for which in range(2):
                    value = sums[u][which]
                    acc[slot % 2, pl.ds(begin + which * pair, pair), :] = value[:pair] + value[pair:]
            return carry

        lax.fori_loop(0, tb // unroll, step, 0)

        def take(which, p, c, ri):
            total = None
            for half in range(2):
                start = which * pair + half * rows_n + (p * cz + c) * 2 + ri
                value = acc[slot % 2, pl.ds(start, tb, stride=quad), :]
                total = value if total is None else total + value
            return total

        for p in range(2):
            for c in range(cz):
                part[slot, p * 2 * cz + c] = take(0, p, c, 0) - take(1, p, c, 1)
                part[slot, (p * 2 + 1) * cz + c] = take(0, p, c, 1) + take(1, p, c, 0)
        if d:
            copy = pltpu.make_async_remote_copy(
                src_ref=part.at[slot],
                dst_ref=recv.at[slot],
                send_sem=part_send.at[slot],
                recv_sem=part_recv.at[slot],
                device_id=peer(lax.rem(tile + d, nt), chan, beam),
                device_id_type=MESH,
            )
            copy.start()
            part_copies.append(copy)

    for copy in part_copies:
        copy.wait_recv()

    def total_of(g, c):
        value = part[nt - 1, g * cz + c]
        for slot in range(nt - 1):
            value = value + recv[slot, g * cz + c]
        return value

    sums = jnp.concatenate(
        [jnp.concatenate([total_of(g, c) for c in range(cz)], axis=1) for g in range(4)], axis=0
    )
    high = sums.astype(BF16)
    low = (sums - high.astype(F32)).astype(BF16)
    table = perm_ref[...]
    moved = jnp.dot(high, table, preferred_element_type=F32) + jnp.dot(
        low, table, preferred_element_type=F32
    )
    group = lax.broadcasted_iota(jnp.int32, (tb, LANES), 1) // fz
    for z in range(nz):
        for c in range(cz):
            total = None
            for g in range(4):
                value = moved[g * tb : (g + 1) * tb, c * LANES : (c + 1) * LANES]
                shift = (g - z) * fz % LANES
                if shift:
                    value = pltpu.roll(value, shift, 1)
                total = value if g == 0 else jnp.where(group == g, value, total)
            packed[z, c] = total

    def pack_copy(h, dz):
        return pltpu.make_async_remote_copy(
            src_ref=packed.at[lax.rem(chan + dz, nz)],
            dst_ref=inbox.at[h, chan],
            send_sem=pack_send.at[h, dz],
            recv_sem=pack_recv.at[h, dz],
            device_id=peer(lax.rem(tile + h, nt), lax.rem(chan + dz, nz), beam),
            device_id_type=MESH,
        )

    spread = sorted(range(nz), key=lambda d: abs(2 * d - nz))
    for h in range(halo + 1):
        for dz in spread:
            if h == 0 and dz == 0:
                continue
            if h == 0:
                pack_copy(h, dz).start()
            else:

                @pl.when(tile + h < nt)
                def _():
                    pack_copy(h, dz).start()

    inbox[0, chan] = packed[chan]

    for copy in tables:
        copy.wait()
    for h in range(halo + 1):
        for dz in range(nz):
            if h == 0 and dz == 0:
                continue
            if h == 0:
                pack_copy(h, dz).wait_recv()
            else:

                @pl.when(tile >= h)
                def _():
                    pack_copy(h, dz).wait_recv()

    lhs = jnp.concatenate(
        [
            jnp.concatenate([inbox[h, z, c] for z in range(nz)], axis=1)
            for c in range(cz)
            for h in range(halo, -1, -1)
        ],
        axis=0,
    )
    high = lhs.astype(BF16)
    low = (lhs - high.astype(F32)).astype(BF16)
    spec[...] = (
        jnp.dot(high, dft_h[...], preferred_element_type=F32)
        + jnp.dot(low, dft_h[...], preferred_element_type=F32)
        + jnp.dot(high, dft_l[...], preferred_element_type=F32)
    )
    span = (halo + 1) * tb
    for c in range(cz):
        for g in range(4):
            total = None
            for k in range(taps):
                value = synth_ref[pl.ds(k, 1), :] * spec[
                    pl.ds(c * span + halo * tb - k, tb), g * LANES : (g + 1) * LANES
                ]
                total = value if total is None else total + value
            out_ref[c, :, g * LANES : (g + 1) * LANES] = total

    for copy in gain_copies:
        copy.wait_send()
    for copy in part_copies:
        copy.wait_send()
    for h in range(halo + 1):
        for dz in range(nz):
            if h == 0 and dz == 0:
                continue
            if h == 0:
                pack_copy(h, dz).wait_send()
            else:

                @pl.when(tile + h < nt)
                def _():
                    pack_copy(h, dz).wait_send()


def rows_of(array):
    lead, width = array.shape[:-2], array.shape[-1]
    split = array.reshape(lead + (2, width // LANES, LANES))
    return jnp.swapaxes(split, -3, -2).reshape(-1, LANES)


def body(mesh, voltages, calib_gain, tile_flags, delays, pointing, synth_filter):
    nt, nz, nb = mesh.shape["tile"], mesh.shape["chan"], mesh.shape["beam"]
    total_rows, n_all = voltages.shape[:2]
    width = voltages.shape[-1]
    taps, k = synth_filter.shape
    tb = total_rows // nt
    fz = width // COARSE
    cz = COARSE // nz
    halo = -(-(taps - 1) // tb)
    n_own = calib_gain.shape[0]
    exchange = n_own % 2 == 0
    gain = calib_gain
    if not exchange:
        gain = gain * tile_flags.astype(F32)[:, None, None, None]
        gain = lax.all_gather(gain, "beam", axis=0, tiled=True)
    rows_n = 4 * cz
    r = np.arange(2 * rows_n)[:, None] % rows_n % (2 * cz) // 2
    local = r * LANES + np.arange(LANES)[None, :]
    channel = (local % COARSE * k + local // COARSE).astype(np.float32)
    dft_h, dft_l = dft_table(nz, fz)
    cfg = (nt, nz, nb, tb, n_all, taps, fz, cz, halo, exchange)
    vmem = pl.BlockSpec(memory_space=pltpu.VMEM)
    smem = pl.BlockSpec(memory_space=pltpu.SMEM)
    anywhere = pl.BlockSpec(memory_space=pl.ANY)
    span = (halo + 1) * tb
    dma = pltpu.SemaphoreType.DMA
    out = pl.pallas_call(
        functools.partial(kernel, cfg),
        out_shape=jax.ShapeDtypeStruct((cz, tb, 4 * k), F32),
        in_specs=[anywhere, vmem, smem, vmem, smem, vmem, vmem, vmem, anywhere, anywhere],
        out_specs=vmem,
        scratch_shapes=[
            pltpu.VMEM((nt, tb * n_all * rows_n, LANES), BF16),
            pltpu.VMEM((nb, n_own * rows_n, LANES), F32),
            pltpu.VMEM((n_all * rows_n, LANES), F32),
            pltpu.VMEM((n_all * rows_n, LANES), F32),
            pltpu.VMEM((2, tb * 4 * rows_n, LANES), F32),
            pltpu.VMEM((nt, 4 * cz, tb, LANES), F32),
            pltpu.VMEM((nt - 1, 4 * cz, tb, LANES), F32),
            pltpu.VMEM((nz, cz, tb, LANES), F32),
            pltpu.VMEM((halo + 1, nz, cz, tb, LANES), F32),
            pltpu.VMEM((cz * span, 4 * k), F32),
            pltpu.VMEM(dft_h.shape, BF16),
            pltpu.VMEM(dft_l.shape, BF16),
            dma((nt,)),
            dma((2,)),
            dma((max(nb - 1, 1),)),
            dma((max(nb - 1, 1),)),
            dma((nt,)),
            dma((nt,)),
            dma((halo + 1, nz)),
            dma((halo + 1, nz)),
        ],
        compiler_params=pltpu.CompilerParams(collective_id=0, has_side_effects=True),
    )(
        rows_of(voltages),
        rows_of(gain),
        tile_flags,
        delays.T,
        pointing,
        synth_filter,
        jnp.asarray(channel),
        jnp.asarray(gather_table(nz, fz, cz)),
        jnp.asarray(dft_h),
        jnp.asarray(dft_l),
    )
    return out.reshape(cz, tb, 2, 2 * k).transpose(1, 2, 0, 3)[:, None]


def solution(mesh):
    in_specs = (
        P(None, "tile", None, None, "chan"),
        P(("tile", "beam"), None, None, "chan"),
        P(("tile", "beam")),
        P(None, "tile"),
        P("beam"),
        P(),
    )
    out_specs = P("tile", "beam", None, "chan", None)
    return jax.shard_map(
        functools.partial(body, mesh), mesh=mesh, in_specs=in_specs, out_specs=out_specs, check_vma=False
    )
```

```python
import functools
import math

import jax
import jax.numpy as jnp
import numpy as np
from jax import lax
from jax.experimental import pallas as pl
from jax.experimental.pallas import tpu as pltpu
from jax.sharding import PartitionSpec as P

COARSE = 12
LANES = 128
MESH = pl.DeviceIdType.MESH
F32 = jnp.float32
BF16 = jnp.bfloat16


def even_fit(func, degree):
    series = np.polynomial.chebyshev.Chebyshev.interpolate(
        lambda u: func(np.sqrt(u)), degree, domain=[0.0, 0.25]
    )
    return [float(v) for v in series.convert(kind=np.polynomial.Polynomial).coef]


COS_COEF = even_fit(lambda r: np.cos(2 * np.pi * r), 7)
SIN_COEF = even_fit(lambda r: 2 * np.pi * np.sinc(2 * r), 7)


def horner(coef, u):
    total = jnp.full_like(u, coef[-1])
    for value in coef[-2::-1]:
        total = total * u + value
    return total


def split_bf16(table):
    high = table.astype(BF16)
    low = (table - high.astype(np.float64)).astype(BF16)
    return high, low


def dft_table(nz, fz):
    k = nz * fz
    f = np.arange(k)
    m = np.arange(k)
    angle = 2 * np.pi * (f[:, None] * m[None, :] % k) / k
    cosine, sine = np.cos(angle) / math.sqrt(k), np.sin(angle) / math.sqrt(k)
    out = np.zeros((nz, 2, 2, fz, 2, 2, k))
    for p in range(2):
        out[:, p, 0, :, p, 0] = cosine.reshape(nz, fz, k)
        out[:, p, 0, :, p, 1] = sine.reshape(nz, fz, k)
        out[:, p, 1, :, p, 0] = -sine.reshape(nz, fz, k)
        out[:, p, 1, :, p, 1] = cosine.reshape(nz, fz, k)
    return split_bf16(out.reshape(nz * 4 * fz, 4 * k))


def gather_table(nz, fz, cz):
    width = fz * COARSE
    out = np.zeros((width, width), np.float64)
    for c in range(cz):
        for z in range(nz):
            for f in range(fz):
                out[f * COARSE + z * cz + c, (c * nz + z) * fz + f] = 1.0
    return out.astype(BF16)


def kernel(
    cfg,
    volt_ref,
    gain_ref,
    flag_ref,
    delay_ref,
    point_ref,
    synth_ref,
    chan_ref,
    perm_ref,
    dfth_ref,
    dftl_ref,
    out_ref,
    volt,
    own_gain,
    gains,
    w_re,
    w_im,
    acc,
    part,
    recv,
    packed,
    inbox,
    spec,
    dft_h,
    dft_l,
    volt_sem,
    table_sem,
    own_sem,
    gain_send,
    gain_recv,
    part_send,
    part_recv,
    pack_send,
    pack_recv,
):
    nt, nz, nb, tb, n_all, taps, fz, cz, halo, exchange = cfg
    tile = lax.axis_index("tile")
    chan = lax.axis_index("chan")
    beam = lax.axis_index("beam")
    rows_t = n_all * 4
    held_t = n_all * 2

    def peer(t, z, b):
        return {"tile": t, "chan": z, "beam": b}

    order = sorted(range(1, nt), key=lambda d: abs(2 * d - nt)) + [0]
    own_loads = [
        pltpu.make_async_copy(
            gain_ref.at[:, :, pl.ds(c * LANES, LANES)], own_gain.at[c], own_sem.at[c]
        )
        for c in range(cz)
    ]
    for load in own_loads:
        load.start()
    loads = []
    for slot, d in enumerate(order):
        block = lax.rem(tile + d, nt)
        loads.append(
            [
                pltpu.make_async_copy(
                    volt_ref.at[pl.ds(block * (tb * held_t), tb * held_t), :, pl.ds(c * LANES, LANES)],
                    volt.at[slot, c],
                    volt_sem.at[slot, c],
                )
                for c in range(cz)
            ]
        )
    for load in loads[0]:
        load.start()
    volt_rows = volt.reshape(nt, cz, tb * rows_t, LANES)
    own_rows = own_gain.reshape(cz, own_gain.shape[1] * 2, LANES)

    barrier = pltpu.get_barrier_semaphore()
    count = 0
    for dt in range(nt):
        for dz in range(nz):
            if dt or dz:
                pl.semaphore_signal(
                    barrier,
                    inc=1,
                    device_id=peer(lax.rem(tile + dt, nt), lax.rem(chan + dz, nz), beam),
                    device_id_type=MESH,
                )
                count += 1
    for db in range(1, nb):
        pl.semaphore_signal(
            barrier, inc=1, device_id=peer(tile, chan, lax.rem(beam + db, nb)), device_id_type=MESH
        )
        count += 1

    for group in loads[1:]:
        for load in group:
            load.start()
    tables = [
        pltpu.make_async_copy(dfth_ref, dft_h, table_sem.at[0]),
        pltpu.make_async_copy(dftl_ref, dft_l, table_sem.at[1]),
    ]
    for copy in tables:
        copy.start()

    row = lax.broadcasted_iota(jnp.int32, (8, LANES), 0)
    first = row < 4
    even = lax.rem(lax.broadcasted_iota(jnp.int32, (rows_t, LANES), 0), 2) == 0
    n_own = n_all // nb

    for load in own_loads:
        load.wait()
    if exchange:
        use = jnp.concatenate(
            [
                jnp.where(first, flag_ref[2 * i].astype(F32), flag_ref[2 * i + 1].astype(F32))
                for i in range(n_own // 2)
            ],
            axis=0,
        )
        for c in range(cz):
            gains[beam, c] = use * own_rows[c]

    for h in range(1, halo + 1):

        @pl.when(tile < h)
        def _():
            inbox[h] = jnp.zeros(inbox.shape[1:], F32)

    pl.semaphore_wait(barrier, count)

    gain_copies = []
    if exchange:
        for db in range(1, nb):
            copy = pltpu.make_async_remote_copy(
                src_ref=gains.at[beam],
                dst_ref=gains.at[beam],
                send_sem=gain_send.at[db - 1],
                recv_sem=gain_recv.at[db - 1],
                device_id=peer(tile, chan, lax.rem(beam + db, nb)),
                device_id_type=MESH,
            )
            copy.start()
            gain_copies.append(copy)

    select = lax.broadcasted_iota(jnp.int32, delay_ref.shape, 1) == point_ref[0]
    delay = jnp.sum(jnp.where(select, delay_ref[...], 0.0), axis=1, keepdims=True)
    delay = jnp.broadcast_to(delay, (n_all, LANES))
    delay = jnp.concatenate(
        [
            jnp.where(
                first,
                jnp.broadcast_to(delay[2 * i : 2 * i + 1], (8, LANES)),
                jnp.broadcast_to(delay[2 * i + 1 : 2 * i + 2], (8, LANES)),
            )
            for i in range(n_all // 2)
        ],
        axis=0,
    )
    for c in range(cz):
        frequency = (chan_ref[pl.ds(c, 1), :] + (chan * fz).astype(F32) + 0.5) / (COARSE * nz * fz)
        cycles = delay * frequency
        turn = cycles - jnp.floor(cycles + 0.5)
        square = turn * turn
        w_re[c] = horner(COS_COEF, square)
        w_im[c] = turn * horner(SIN_COEF, square)

    for copy in gain_copies:
        copy.wait_recv()

    for c in range(cz):
        if exchange:
            gain = jnp.concatenate([gains[b, c] for b in range(nb)], axis=0)
        else:
            gain = own_rows[c]
        swapped = jnp.where(even, pltpu.roll(gain, rows_t - 1, 0), -pltpu.roll(gain, 1, 0))
        weight = gain * w_re[c] + swapped * w_im[c]
        w_re[c] = jnp.where(even, weight, pltpu.roll(weight, 1, 0))
        w_im[c] = jnp.where(even, pltpu.roll(weight, rows_t - 1, 0), weight)

    unroll = 2
    kept = cz * 2 * 8
    part_copies = []
    for slot, d in enumerate(order):
        for load in loads[slot]:
            load.wait()

        def step(s, carry):
            for c in range(cz):
                sums = [[jnp.zeros((16, LANES), F32)] * 2 for _ in range(unroll)]
                for q in range(rows_t // 16):
                    wr = w_re[c, pl.ds(q * 16, 16), :]
                    wi = w_im[c, pl.ds(q * 16, 16), :]
                    for u in range(unroll):
                        begin = pl.multiple_of((s * unroll + u) * rows_t, 16) + q * 16
                        v = volt_rows[slot, c, pl.ds(begin, 16), :].astype(F32)
                        sums[u] = [sums[u][0] + wr * v, sums[u][1] + wi * v]
                for u in range(unroll):
                    begin = pl.multiple_of((s * unroll + u) * kept, 8)
                    for which in range(2):
                        value = sums[u][which]
                        acc[slot % 2, pl.ds(begin + (c * 2 + which) * 8, 8), :] = value[:8] + value[8:]
            return carry

        lax.fori_loop(0, tb // unroll, step, 0)

        def take(which, p, c, ri):
            total = None
            for half in range(2):
                start = (c * 2 + which) * 8 + half * 4 + p * 2 + ri
                value = acc[slot % 2, pl.ds(start, tb, stride=kept), :]
                total = value if total is None else total + value
            return total

        for p in range(2):
            for c in range(cz):
                part[slot, p * 2 * cz + c] = take(0, p, c, 0) - take(1, p, c, 1)
                part[slot, (p * 2 + 1) * cz + c] = take(0, p, c, 1) + take(1, p, c, 0)
        if d:
            copy = pltpu.make_async_remote_copy(
                src_ref=part.at[slot],
                dst_ref=recv.at[slot],
                send_sem=part_send.at[slot],
                recv_sem=part_recv.at[slot],
                device_id=peer(lax.rem(tile + d, nt), chan, beam),
                device_id_type=MESH,
            )
            copy.start()
            part_copies.append(copy)

    for copy in part_copies:
        copy.wait_recv()

    def total_of(g, c):
        value = part[nt - 1, g * cz + c]
        for slot in range(nt - 1):
            value = value + recv[slot, g * cz + c]
        return value

    sums = jnp.concatenate(
        [jnp.concatenate([total_of(g, c) for c in range(cz)], axis=1) for g in range(4)], axis=0
    )
    high = sums.astype(BF16)
    low = (sums - high.astype(F32)).astype(BF16)
    table = perm_ref[...]
    moved = jnp.dot(high, table, preferred_element_type=F32) + jnp.dot(
        low, table, preferred_element_type=F32
    )
    group = lax.broadcasted_iota(jnp.int32, (tb, LANES), 1) // fz
    for z in range(nz):
        for c in range(cz):
            total = None
            for g in range(4):
                value = moved[g * tb : (g + 1) * tb, c * LANES : (c + 1) * LANES]
                shift = (g - z) * fz % LANES
                if shift:
                    value = pltpu.roll(value, shift, 1)
                total = value if g == 0 else jnp.where(group == g, value, total)
            packed[z, c] = total

    def pack_copy(h, dz):
        return pltpu.make_async_remote_copy(
            src_ref=packed.at[lax.rem(chan + dz, nz)],
            dst_ref=inbox.at[h, chan],
            send_sem=pack_send.at[h, dz],
            recv_sem=pack_recv.at[h, dz],
            device_id=peer(lax.rem(tile + h, nt), lax.rem(chan + dz, nz), beam),
            device_id_type=MESH,
        )

    spread = sorted(range(nz), key=lambda d: abs(2 * d - nz))
    for h in range(halo + 1):
        for dz in spread:
            if h == 0 and dz == 0:
                continue
            if h == 0:
                pack_copy(h, dz).start()
            else:

                @pl.when(tile + h < nt)
                def _():
                    pack_copy(h, dz).start()

    inbox[0, chan] = packed[chan]

    for copy in tables:
        copy.wait()
    for h in range(halo + 1):
        for dz in range(nz):
            if h == 0 and dz == 0:
                continue
            if h == 0:
                pack_copy(h, dz).wait_recv()
            else:

                @pl.when(tile >= h)
                def _():
                    pack_copy(h, dz).wait_recv()

    lhs = jnp.concatenate(
        [
            jnp.concatenate([inbox[h, z, c] for z in range(nz)], axis=1)
            for c in range(cz)
            for h in range(halo, -1, -1)
        ],
        axis=0,
    )
    high = lhs.astype(BF16)
    low = (lhs - high.astype(F32)).astype(BF16)
    spec[...] = (
        jnp.dot(high, dft_h[...], preferred_element_type=F32)
        + jnp.dot(low, dft_h[...], preferred_element_type=F32)
        + jnp.dot(high, dft_l[...], preferred_element_type=F32)
    )
    span = (halo + 1) * tb
    for c in range(cz):
        for g in range(4):
            total = None
            for k in range(taps):
                value = synth_ref[pl.ds(k, 1), :] * spec[
                    pl.ds(c * span + halo * tb - k, tb), g * LANES : (g + 1) * LANES
                ]
                total = value if total is None else total + value
            out_ref[c, :, g * LANES : (g + 1) * LANES] = total

    for copy in gain_copies:
        copy.wait_send()
    for copy in part_copies:
        copy.wait_send()
    for h in range(halo + 1):
        for dz in range(nz):
            if h == 0 and dz == 0:
                continue
            if h == 0:
                pack_copy(h, dz).wait_send()
            else:

                @pl.when(tile + h < nt)
                def _():
                    pack_copy(h, dz).wait_send()


def body(mesh, voltages, calib_gain, tile_flags, delays, pointing, synth_filter):
    nt, nz, nb = mesh.shape["tile"], mesh.shape["chan"], mesh.shape["beam"]
    total_rows, n_all = voltages.shape[:2]
    width = voltages.shape[-1]
    taps, k = synth_filter.shape
    tb = total_rows // nt
    fz = width // COARSE
    cz = COARSE // nz
    halo = -(-(taps - 1) // tb)
    n_own = calib_gain.shape[0]
    exchange = n_own % 2 == 0
    gain = calib_gain
    if not exchange:
        gain = gain * tile_flags.astype(F32)[:, None, None, None]
        gain = lax.all_gather(gain, "beam", axis=0, tiled=True)
    local = np.arange(width).reshape(-1, LANES)
    channel = (local % COARSE * k + local // COARSE).astype(np.float32)
    dft_h, dft_l = dft_table(nz, fz)
    cfg = (nt, nz, nb, tb, n_all, taps, fz, cz, halo, exchange)
    vmem = pl.BlockSpec(memory_space=pltpu.VMEM)
    smem = pl.BlockSpec(memory_space=pltpu.SMEM)
    anywhere = pl.BlockSpec(memory_space=pl.ANY)
    span = (halo + 1) * tb
    dma = pltpu.SemaphoreType.DMA
    out = pl.pallas_call(
        functools.partial(kernel, cfg),
        out_shape=jax.ShapeDtypeStruct((cz, tb, 4 * k), F32),
        in_specs=[anywhere, anywhere, smem, vmem, smem, vmem, vmem, vmem, anywhere, anywhere],
        out_specs=vmem,
        scratch_shapes=[
            pltpu.VMEM((nt, cz, tb * n_all * 2, 2, LANES), BF16),
            pltpu.VMEM((cz, gain.shape[0] * 2, 2, LANES), F32),
            pltpu.VMEM((nb, cz, n_own * 4, LANES), F32),
            pltpu.VMEM((cz, n_all * 4, LANES), F32),
            pltpu.VMEM((cz, n_all * 4, LANES), F32),
            pltpu.VMEM((2, tb * cz * 16, LANES), F32),
            pltpu.VMEM((nt, 4 * cz, tb, LANES), F32),
            pltpu.VMEM((nt - 1, 4 * cz, tb, LANES), F32),
            pltpu.VMEM((nz, cz, tb, LANES), F32),
            pltpu.VMEM((halo + 1, nz, cz, tb, LANES), F32),
            pltpu.VMEM((cz * span, 4 * k), F32),
            pltpu.VMEM(dft_h.shape, BF16),
            pltpu.VMEM(dft_l.shape, BF16),
            dma((nt, cz)),
            dma((2,)),
            dma((cz,)),
            dma((max(nb - 1, 1),)),
            dma((max(nb - 1, 1),)),
            dma((nt,)),
            dma((nt,)),
            dma((halo + 1, nz)),
            dma((halo + 1, nz)),
        ],
        compiler_params=pltpu.CompilerParams(collective_id=0, has_side_effects=True),
    )(
        voltages.reshape(-1, 2, width),
        gain.reshape(-1, 2, width),
        tile_flags,
        delays.T,
        pointing,
        synth_filter,
        jnp.asarray(channel),
        jnp.asarray(gather_table(nz, fz, cz)),
        jnp.asarray(dft_h),
        jnp.asarray(dft_l),
    )
    return out.reshape(cz, tb, 2, 2 * k).transpose(1, 2, 0, 3)[:, None]


def solution(mesh):
    in_specs = (
        P(None, "tile", None, None, "chan"),
        P(("tile", "beam"), None, None, "chan"),
        P(("tile", "beam")),
        P(None, "tile"),
        P("beam"),
        P(),
    )
    out_specs = P("tile", "beam", None, "chan", None)
    return jax.shard_map(
        functools.partial(body, mesh), mesh=mesh, in_specs=in_specs, out_specs=out_specs, check_vma=False
    )
```

```python
import functools
import math

import jax
import jax.numpy as jnp
import numpy as np
from jax import lax
from jax.experimental import pallas as pl
from jax.experimental.pallas import tpu as pltpu
from jax.sharding import PartitionSpec as P

COARSE = 12
LANES = 128
MESH = pl.DeviceIdType.MESH
F32 = jnp.float32
BF16 = jnp.bfloat16


def even_fit(func, degree):
    series = np.polynomial.chebyshev.Chebyshev.interpolate(
        lambda u: func(np.sqrt(u)), degree, domain=[0.0, 0.25]
    )
    return [float(v) for v in series.convert(kind=np.polynomial.Polynomial).coef]


COS_COEF = even_fit(lambda r: np.cos(2 * np.pi * r), 7)
SIN_COEF = even_fit(lambda r: 2 * np.pi * np.sinc(2 * r), 7)


def horner(coef, u):
    total = jnp.full_like(u, coef[-1])
    for value in coef[-2::-1]:
        total = total * u + value
    return total


def split_bf16(table):
    high = table.astype(BF16)
    low = (table - high.astype(np.float64)).astype(BF16)
    return high, low


def dft_table(nz, fz):
    k = nz * fz
    f = np.arange(k)
    m = np.arange(k)
    angle = 2 * np.pi * (f[:, None] * m[None, :] % k) / k
    cosine, sine = np.cos(angle) / math.sqrt(k), np.sin(angle) / math.sqrt(k)
    out = np.zeros((nz, 2, 2, fz, 2, 2, k))
    for p in range(2):
        out[:, p, 0, :, p, 0] = cosine.reshape(nz, fz, k)
        out[:, p, 0, :, p, 1] = sine.reshape(nz, fz, k)
        out[:, p, 1, :, p, 0] = -sine.reshape(nz, fz, k)
        out[:, p, 1, :, p, 1] = cosine.reshape(nz, fz, k)
    return split_bf16(out.reshape(nz * 4 * fz, 4 * k))


def gather_table(nz, fz, cz):
    width = fz * COARSE
    out = np.zeros((width, width), np.float64)
    for c in range(cz):
        for z in range(nz):
            for f in range(fz):
                out[f * COARSE + z * cz + c, (c * nz + z) * fz + f] = 1.0
    return out.astype(BF16)


def kernel(
    cfg,
    volt_ref,
    gain_ref,
    flag_src,
    delay_src,
    point_src,
    synth_src,
    chan_src,
    perm_src,
    dfth_ref,
    dftl_ref,
    out_ref,
    flag_ref,
    delay_ref,
    point_ref,
    synth_ref,
    chan_ref,
    perm_ref,
    small_sem,
    volt,
    own_gain,
    gains,
    w_re,
    w_im,
    acc,
    part,
    recv,
    packed,
    inbox,
    spec,
    dft_h,
    dft_l,
    volt_sem,
    table_sem,
    own_sem,
    gain_send,
    gain_recv,
    part_send,
    part_recv,
    pack_send,
    pack_recv,
):
    nt, nz, nb, tb, n_all, taps, fz, cz, halo, exchange = cfg
    tile = lax.axis_index("tile")
    chan = lax.axis_index("chan")
    beam = lax.axis_index("beam")
    rows_t = n_all * 4
    held_t = n_all * 2

    def peer(t, z, b):
        return {"tile": t, "chan": z, "beam": b}

    order = sorted(range(1, nt), key=lambda d: abs(2 * d - nt)) + [0]
    barrier = pltpu.get_barrier_semaphore()
    count = 0
    for dt in range(nt):
        for dz in range(nz):
            if dt or dz:
                pl.semaphore_signal(
                    barrier,
                    inc=1,
                    device_id=peer(lax.rem(tile + dt, nt), lax.rem(chan + dz, nz), beam),
                    device_id_type=MESH,
                )
                count += 1
    for db in range(1, nb):
        pl.semaphore_signal(
            barrier, inc=1, device_id=peer(tile, chan, lax.rem(beam + db, nb)), device_id_type=MESH
        )
        count += 1

    small = [
        pltpu.make_async_copy(src, dst, small_sem.at[i])
        for i, (src, dst) in enumerate(
            [
                (flag_src, flag_ref),
                (point_src, point_ref),
                (delay_src, delay_ref),
                (chan_src, chan_ref),
                (synth_src, synth_ref),
                (perm_src, perm_ref),
            ]
        )
    ]
    own_loads = [
        pltpu.make_async_copy(
            gain_ref.at[:, :, pl.ds(c * LANES, LANES)], own_gain.at[c], own_sem.at[c]
        )
        for c in range(cz)
    ]
    for load in own_loads + small[:4]:
        load.start()
    loads = []
    for slot, d in enumerate(order):
        block = lax.rem(tile + d, nt)
        loads.append(
            [
                pltpu.make_async_copy(
                    volt_ref.at[pl.ds(block * (tb * held_t), tb * held_t), :, pl.ds(c * LANES, LANES)],
                    volt.at[slot, c],
                    volt_sem.at[slot, c],
                )
                for c in range(cz)
            ]
        )
    for load in loads[0]:
        load.start()
    volt_rows = volt.reshape(nt, cz, tb * rows_t, LANES)
    own_rows = own_gain.reshape(cz, own_gain.shape[1] * 2, LANES)

    for group in loads[1:]:
        for load in group:
            load.start()
    tables = [
        pltpu.make_async_copy(dfth_ref, dft_h, table_sem.at[0]),
        pltpu.make_async_copy(dftl_ref, dft_l, table_sem.at[1]),
    ]
    for copy in small[4:] + tables:
        copy.start()

    row = lax.broadcasted_iota(jnp.int32, (8, LANES), 0)
    first = row < 4
    even = lax.rem(lax.broadcasted_iota(jnp.int32, (rows_t, LANES), 0), 2) == 0
    n_own = n_all // nb

    for load in own_loads + small[:1]:
        load.wait()
    if exchange:
        use = jnp.concatenate(
            [
                jnp.where(first, flag_ref[2 * i].astype(F32), flag_ref[2 * i + 1].astype(F32))
                for i in range(n_own // 2)
            ],
            axis=0,
        )
        for c in range(cz):
            gains[beam, c] = use * own_rows[c]

    for h in range(1, halo + 1):

        @pl.when(tile < h)
        def _():
            inbox[h] = jnp.zeros(inbox.shape[1:], F32)

    pl.semaphore_wait(barrier, count)

    gain_copies = []
    if exchange:
        for db in range(1, nb):
            copy = pltpu.make_async_remote_copy(
                src_ref=gains.at[beam],
                dst_ref=gains.at[beam],
                send_sem=gain_send.at[db - 1],
                recv_sem=gain_recv.at[db - 1],
                device_id=peer(tile, chan, lax.rem(beam + db, nb)),
                device_id_type=MESH,
            )
            copy.start()
            gain_copies.append(copy)

    for copy in small[1:4]:
        copy.wait()
    select = lax.broadcasted_iota(jnp.int32, delay_ref.shape, 1) == point_ref[0]
    delay = jnp.sum(jnp.where(select, delay_ref[...], 0.0), axis=1, keepdims=True)
    delay = jnp.broadcast_to(delay, (n_all, LANES))
    delay = jnp.concatenate(
        [
            jnp.where(
                first,
                jnp.broadcast_to(delay[2 * i : 2 * i + 1], (8, LANES)),
                jnp.broadcast_to(delay[2 * i + 1 : 2 * i + 2], (8, LANES)),
            )
            for i in range(n_all // 2)
        ],
        axis=0,
    )
    for c in range(cz):
        frequency = (chan_ref[pl.ds(c, 1), :] + (chan * fz).astype(F32) + 0.5) / (COARSE * nz * fz)
        cycles = delay * frequency
        turn = cycles - jnp.floor(cycles + 0.5)
        square = turn * turn
        w_re[c] = horner(COS_COEF, square)
        w_im[c] = turn * horner(SIN_COEF, square)

    for copy in gain_copies:
        copy.wait_recv()

    for c in range(cz):
        if exchange:
            gain = jnp.concatenate([gains[b, c] for b in range(nb)], axis=0)
        else:
            gain = own_rows[c]
        swapped = jnp.where(even, pltpu.roll(gain, rows_t - 1, 0), -pltpu.roll(gain, 1, 0))
        weight = gain * w_re[c] + swapped * w_im[c]
        w_re[c] = jnp.where(even, weight, pltpu.roll(weight, 1, 0))
        w_im[c] = jnp.where(even, pltpu.roll(weight, rows_t - 1, 0), weight)

    unroll = 2
    kept = cz * 2 * 8
    part_copies = []
    for slot, d in enumerate(order):
        for load in loads[slot]:
            load.wait()

        def step(s, carry):
            for c in range(cz):
                sums = [[jnp.zeros((16, LANES), F32)] * 2 for _ in range(unroll)]
                for q in range(rows_t // 16):
                    wr = w_re[c, pl.ds(q * 16, 16), :]
                    wi = w_im[c, pl.ds(q * 16, 16), :]
                    for u in range(unroll):
                        begin = pl.multiple_of((s * unroll + u) * rows_t, 16) + q * 16
                        v = volt_rows[slot, c, pl.ds(begin, 16), :].astype(F32)
                        sums[u] = [sums[u][0] + wr * v, sums[u][1] + wi * v]
                for u in range(unroll):
                    begin = pl.multiple_of((s * unroll + u) * kept, 8)
                    for which in range(2):
                        value = sums[u][which]
                        acc[slot % 2, pl.ds(begin + (c * 2 + which) * 8, 8), :] = value[:8] + value[8:]
            return carry

        lax.fori_loop(0, tb // unroll, step, 0)

        def take(which, p, c, ri):
            total = None
            for half in range(2):
                start = (c * 2 + which) * 8 + half * 4 + p * 2 + ri
                value = acc[slot % 2, pl.ds(start, tb, stride=kept), :]
                total = value if total is None else total + value
            return total

        for p in range(2):
            for c in range(cz):
                part[slot, p * 2 * cz + c] = take(0, p, c, 0) - take(1, p, c, 1)
                part[slot, (p * 2 + 1) * cz + c] = take(0, p, c, 1) + take(1, p, c, 0)
        if d:
            copy = pltpu.make_async_remote_copy(
                src_ref=part.at[slot],
                dst_ref=recv.at[slot],
                send_sem=part_send.at[slot],
                recv_sem=part_recv.at[slot],
                device_id=peer(lax.rem(tile + d, nt), chan, beam),
                device_id_type=MESH,
            )
            copy.start()
            part_copies.append(copy)

    for copy in part_copies:
        copy.wait_recv()

    def total_of(g, c):
        value = part[nt - 1, g * cz + c]
        for slot in range(nt - 1):
            value = value + recv[slot, g * cz + c]
        return value

    sums = jnp.concatenate(
        [jnp.concatenate([total_of(g, c) for c in range(cz)], axis=1) for g in range(4)], axis=0
    )
    high = sums.astype(BF16)
    low = (sums - high.astype(F32)).astype(BF16)
    for copy in small[4:]:
        copy.wait()
    table = perm_ref[...]
    moved = jnp.dot(high, table, preferred_element_type=F32) + jnp.dot(
        low, table, preferred_element_type=F32
    )
    group = lax.broadcasted_iota(jnp.int32, (tb, LANES), 1) // fz
    for z in range(nz):
        for c in range(cz):
            total = None
            for g in range(4):
                value = moved[g * tb : (g + 1) * tb, c * LANES : (c + 1) * LANES]
                shift = (g - z) * fz % LANES
                if shift:
                    value = pltpu.roll(value, shift, 1)
                total = value if g == 0 else jnp.where(group == g, value, total)
            packed[z, c] = total

    def pack_copy(h, dz):
        return pltpu.make_async_remote_copy(
            src_ref=packed.at[lax.rem(chan + dz, nz)],
            dst_ref=inbox.at[h, chan],
            send_sem=pack_send.at[h, dz],
            recv_sem=pack_recv.at[h, dz],
            device_id=peer(lax.rem(tile + h, nt), lax.rem(chan + dz, nz), beam),
            device_id_type=MESH,
        )

    spread = sorted(range(nz), key=lambda d: abs(2 * d - nz))
    for h in range(halo + 1):
        for dz in spread:
            if h == 0 and dz == 0:
                continue
            if h == 0:
                pack_copy(h, dz).start()
            else:

                @pl.when(tile + h < nt)
                def _():
                    pack_copy(h, dz).start()

    inbox[0, chan] = packed[chan]

    for copy in tables:
        copy.wait()
    for h in range(halo + 1):
        for dz in range(nz):
            if h == 0 and dz == 0:
                continue
            if h == 0:
                pack_copy(h, dz).wait_recv()
            else:

                @pl.when(tile >= h)
                def _():
                    pack_copy(h, dz).wait_recv()

    lhs = jnp.concatenate(
        [
            jnp.concatenate([inbox[h, z, c] for z in range(nz)], axis=1)
            for c in range(cz)
            for h in range(halo, -1, -1)
        ],
        axis=0,
    )
    high = lhs.astype(BF16)
    low = (lhs - high.astype(F32)).astype(BF16)
    spec[...] = (
        jnp.dot(high, dft_h[...], preferred_element_type=F32)
        + jnp.dot(low, dft_h[...], preferred_element_type=F32)
        + jnp.dot(high, dft_l[...], preferred_element_type=F32)
    )
    span = (halo + 1) * tb
    for c in range(cz):
        for g in range(4):
            total = None
            for k in range(taps):
                value = synth_ref[pl.ds(k, 1), :] * spec[
                    pl.ds(c * span + halo * tb - k, tb), g * LANES : (g + 1) * LANES
                ]
                total = value if total is None else total + value
            out_ref[c, :, g * LANES : (g + 1) * LANES] = total

    for copy in gain_copies:
        copy.wait_send()
    for copy in part_copies:
        copy.wait_send()
    for h in range(halo + 1):
        for dz in range(nz):
            if h == 0 and dz == 0:
                continue
            if h == 0:
                pack_copy(h, dz).wait_send()
            else:

                @pl.when(tile + h < nt)
                def _():
                    pack_copy(h, dz).wait_send()


def body(mesh, voltages, calib_gain, tile_flags, delays, pointing, synth_filter):
    nt, nz, nb = mesh.shape["tile"], mesh.shape["chan"], mesh.shape["beam"]
    total_rows, n_all = voltages.shape[:2]
    width = voltages.shape[-1]
    taps, k = synth_filter.shape
    tb = total_rows // nt
    fz = width // COARSE
    cz = COARSE // nz
    halo = -(-(taps - 1) // tb)
    n_own = calib_gain.shape[0]
    exchange = n_own % 2 == 0
    gain = calib_gain
    if not exchange:
        gain = gain * tile_flags.astype(F32)[:, None, None, None]
        gain = lax.all_gather(gain, "beam", axis=0, tiled=True)
    local = np.arange(width).reshape(-1, LANES)
    channel = (local % COARSE * k + local // COARSE).astype(np.float32)
    dft_h, dft_l = dft_table(nz, fz)
    perm = gather_table(nz, fz, cz)
    cfg = (nt, nz, nb, tb, n_all, taps, fz, cz, halo, exchange)
    vmem = pl.BlockSpec(memory_space=pltpu.VMEM)
    anywhere = pl.BlockSpec(memory_space=pl.ANY)
    span = (halo + 1) * tb
    dma = pltpu.SemaphoreType.DMA
    out = pl.pallas_call(
        functools.partial(kernel, cfg),
        out_shape=jax.ShapeDtypeStruct((cz, tb, 4 * k), F32),
        in_specs=[anywhere] * 10,
        out_specs=vmem,
        scratch_shapes=[
            pltpu.SMEM(tile_flags.shape, jnp.int32),
            pltpu.VMEM(delays.shape[::-1], F32),
            pltpu.SMEM(pointing.shape, jnp.int32),
            pltpu.VMEM(synth_filter.shape, F32),
            pltpu.VMEM(channel.shape, F32),
            pltpu.VMEM(perm.shape, BF16),
            dma((6,)),
            pltpu.VMEM((nt, cz, tb * n_all * 2, 2, LANES), BF16),
            pltpu.VMEM((cz, gain.shape[0] * 2, 2, LANES), F32),
            pltpu.VMEM((nb, cz, n_own * 4, LANES), F32),
            pltpu.VMEM((cz, n_all * 4, LANES), F32),
            pltpu.VMEM((cz, n_all * 4, LANES), F32),
            pltpu.VMEM((2, tb * cz * 16, LANES), F32),
            pltpu.VMEM((nt, 4 * cz, tb, LANES), F32),
            pltpu.VMEM((nt - 1, 4 * cz, tb, LANES), F32),
            pltpu.VMEM((nz, cz, tb, LANES), F32),
            pltpu.VMEM((halo + 1, nz, cz, tb, LANES), F32),
            pltpu.VMEM((cz * span, 4 * k), F32),
            pltpu.VMEM(dft_h.shape, BF16),
            pltpu.VMEM(dft_l.shape, BF16),
            dma((nt, cz)),
            dma((2,)),
            dma((cz,)),
            dma((max(nb - 1, 1),)),
            dma((max(nb - 1, 1),)),
            dma((nt,)),
            dma((nt,)),
            dma((halo + 1, nz)),
            dma((halo + 1, nz)),
        ],
        compiler_params=pltpu.CompilerParams(collective_id=0, has_side_effects=True),
    )(
        voltages.reshape(-1, 2, width),
        gain.reshape(-1, 2, width),
        tile_flags,
        delays.T,
        pointing,
        synth_filter,
        jnp.asarray(channel),
        jnp.asarray(perm),
        jnp.asarray(dft_h),
        jnp.asarray(dft_l),
    )
    return out.reshape(cz, tb, 2, 2 * k).transpose(1, 2, 0, 3)[:, None]


def solution(mesh):
    in_specs = (
        P(None, "tile", None, None, "chan"),
        P(("tile", "beam"), None, None, "chan"),
        P(("tile", "beam")),
        P(None, "tile"),
        P("beam"),
        P(),
    )
    out_specs = P("tile", "beam", None, "chan", None)
    return jax.shard_map(
        functools.partial(body, mesh), mesh=mesh, in_specs=in_specs, out_specs=out_specs, check_vma=False
    )
```

```python
import functools
import math

import jax
import jax.numpy as jnp
import numpy as np
from jax import lax
from jax.experimental import pallas as pl
from jax.experimental.pallas import tpu as pltpu
from jax.sharding import PartitionSpec as P

COARSE = 12
LANES = 128
MESH = pl.DeviceIdType.MESH
F32 = jnp.float32
BF16 = jnp.bfloat16


def even_fit(func, degree):
    series = np.polynomial.chebyshev.Chebyshev.interpolate(
        lambda u: func(np.sqrt(u)), degree, domain=[0.0, 0.25]
    )
    return [float(v) for v in series.convert(kind=np.polynomial.Polynomial).coef]


COS_COEF = even_fit(lambda r: np.cos(2 * np.pi * r), 7)
SIN_COEF = even_fit(lambda r: 2 * np.pi * np.sinc(2 * r), 7)


def horner(coef, u):
    total = jnp.full_like(u, coef[-1])
    for value in coef[-2::-1]:
        total = total * u + value
    return total


def split_bf16(table):
    high = table.astype(BF16)
    low = (table - high.astype(np.float64)).astype(BF16)
    return high, low


def dft_table(nz, fz):
    k = nz * fz
    f = np.arange(k)
    m = np.arange(k)
    angle = 2 * np.pi * (f[:, None] * m[None, :] % k) / k
    cosine, sine = np.cos(angle) / math.sqrt(k), np.sin(angle) / math.sqrt(k)
    out = np.zeros((nz, 2, 2, fz, 2, 2, k))
    for p in range(2):
        out[:, p, 0, :, p, 0] = cosine.reshape(nz, fz, k)
        out[:, p, 0, :, p, 1] = sine.reshape(nz, fz, k)
        out[:, p, 1, :, p, 0] = -sine.reshape(nz, fz, k)
        out[:, p, 1, :, p, 1] = cosine.reshape(nz, fz, k)
    return split_bf16(out.reshape(nz * 4 * fz, 4 * k))


def gather_table(nz, fz, cz):
    width = fz * COARSE
    out = np.zeros((width, width), np.float64)
    for c in range(cz):
        for z in range(nz):
            for f in range(fz):
                out[f * COARSE + z * cz + c, (c * nz + z) * fz + f] = 1.0
    return out.astype(BF16)


def kernel(
    cfg,
    volt_ref,
    gain_ref,
    flag_src,
    delay_src,
    point_src,
    synth_src,
    chan_src,
    perm_src,
    dfth_ref,
    dftl_ref,
    out_ref,
    flag_ref,
    delay_ref,
    point_ref,
    synth_ref,
    chan_ref,
    perm_ref,
    small_sem,
    volt,
    own_gain,
    gains,
    w_re,
    w_im,
    acc,
    part,
    recv,
    packed,
    inbox,
    spec,
    dft_h,
    dft_l,
    volt_sem,
    table_sem,
    own_sem,
    gain_send,
    gain_recv,
    part_send,
    part_recv,
    pack_send,
    pack_recv,
):
    nt, nz, nb, tb, n_all, taps, fz, cz, halo, exchange = cfg
    tile = lax.axis_index("tile")
    chan = lax.axis_index("chan")
    beam = lax.axis_index("beam")
    rows_t = n_all * 4
    held_t = n_all * 2

    def peer(t, z, b):
        return {"tile": t, "chan": z, "beam": b}

    order = sorted(range(1, nt), key=lambda d: abs(2 * d - nt)) + [0]
    barrier = pltpu.get_barrier_semaphore()
    count = 0
    for dt in range(nt):
        for dz in range(nz):
            if dt or dz:
                pl.semaphore_signal(
                    barrier,
                    inc=1,
                    device_id=peer(lax.rem(tile + dt, nt), lax.rem(chan + dz, nz), beam),
                    device_id_type=MESH,
                )
                count += 1
    for db in range(1, nb):
        pl.semaphore_signal(
            barrier, inc=1, device_id=peer(tile, chan, lax.rem(beam + db, nb)), device_id_type=MESH
        )
        count += 1

    small = [
        pltpu.make_async_copy(src, dst, small_sem.at[i])
        for i, (src, dst) in enumerate(
            [
                (flag_src, flag_ref),
                (point_src, point_ref),
                (delay_src, delay_ref),
                (chan_src, chan_ref),
                (synth_src, synth_ref),
                (perm_src, perm_ref),
            ]
        )
    ]
    own_loads = [
        pltpu.make_async_copy(
            gain_ref.at[:, :, pl.ds(c * LANES, LANES)], own_gain.at[c], own_sem.at[c]
        )
        for c in range(cz)
    ]
    for load in own_loads + small[:4]:
        load.start()
    loads = []
    for slot, d in enumerate(order):
        block = lax.rem(tile + d, nt)
        loads.append(
            [
                pltpu.make_async_copy(
                    volt_ref.at[pl.ds(block * (tb * held_t), tb * held_t), :, pl.ds(c * LANES, LANES)],
                    volt.at[slot, c],
                    volt_sem.at[slot, c],
                )
                for c in range(cz)
            ]
        )
    for load in loads[0]:
        load.start()
    volt_rows = volt.reshape(nt, cz, tb * rows_t, LANES)
    own_rows = own_gain.reshape(cz, own_gain.shape[1] * 2, LANES)

    for group in loads[1:]:
        for load in group:
            load.start()
    tables = [
        pltpu.make_async_copy(dfth_ref, dft_h, table_sem.at[0]),
        pltpu.make_async_copy(dftl_ref, dft_l, table_sem.at[1]),
    ]
    for copy in small[4:] + tables:
        copy.start()

    row = lax.broadcasted_iota(jnp.int32, (8, LANES), 0)
    first = row < 4
    n_own = n_all // nb
    share = n_own * 4 if exchange else rows_t
    even = lax.rem(lax.broadcasted_iota(jnp.int32, (share, LANES), 0), 2) == 0

    for load in own_loads + small[:1]:
        load.wait()
    if exchange:
        use = jnp.concatenate(
            [
                jnp.where(first, flag_ref[2 * i].astype(F32), flag_ref[2 * i + 1].astype(F32))
                for i in range(n_own // 2)
            ],
            axis=0,
        )
        for c in range(cz):
            gains[beam, c] = use * own_rows[c]

    for h in range(1, halo + 1):

        @pl.when(tile < h)
        def _():
            inbox[h] = jnp.zeros(inbox.shape[1:], F32)

    pl.semaphore_wait(barrier, count)

    gain_copies = []
    if exchange:
        for db in range(1, nb):
            copy = pltpu.make_async_remote_copy(
                src_ref=gains.at[beam],
                dst_ref=gains.at[beam],
                send_sem=gain_send.at[db - 1],
                recv_sem=gain_recv.at[db - 1],
                device_id=peer(tile, chan, lax.rem(beam + db, nb)),
                device_id_type=MESH,
            )
            copy.start()
            gain_copies.append(copy)

    for copy in small[1:4]:
        copy.wait()
    select = lax.broadcasted_iota(jnp.int32, delay_ref.shape, 1) == point_ref[0]
    delay = jnp.sum(jnp.where(select, delay_ref[...], 0.0), axis=1, keepdims=True)
    delay = jnp.broadcast_to(delay, (n_all, LANES))
    delay = jnp.concatenate(
        [
            jnp.where(
                first,
                jnp.broadcast_to(delay[2 * i : 2 * i + 1], (8, LANES)),
                jnp.broadcast_to(delay[2 * i + 1 : 2 * i + 2], (8, LANES)),
            )
            for i in range(n_all // 2)
        ],
        axis=0,
    )
    for c in range(cz):
        frequency = (chan_ref[pl.ds(c, 1), :] + (chan * fz).astype(F32) + 0.5) / (COARSE * nz * fz)
        cycles = delay * frequency
        turn = cycles - jnp.floor(cycles + 0.5)
        square = turn * turn
        w_re[c] = horner(COS_COEF, square)
        w_im[c] = turn * horner(SIN_COEF, square)

    def weigh(start, gain_of):
        rows = pl.ds(start, share)
        for c in range(cz):
            gain = gain_of(c)
            swapped = jnp.where(even, pltpu.roll(gain, share - 1, 0), -pltpu.roll(gain, 1, 0))
            weight = gain * w_re[c, rows, :] + swapped * w_im[c, rows, :]
            w_re[c, rows, :] = jnp.where(even, weight, pltpu.roll(weight, 1, 0))
            w_im[c, rows, :] = jnp.where(even, pltpu.roll(weight, share - 1, 0), weight)

    unroll = 2
    kept = cz * 2 * 8

    def accumulate(slot, starts, extend):
        def step(s, carry):
            for c in range(cz):
                sums = [[jnp.zeros((16, LANES), F32)] * 2 for _ in range(unroll)]
                for start in starts:
                    for q in range(share // 16):
                        at = start + q * 16
                        wr = w_re[c, pl.ds(at, 16), :]
                        wi = w_im[c, pl.ds(at, 16), :]
                        for u in range(unroll):
                            begin = pl.multiple_of((s * unroll + u) * rows_t + at, 16)
                            v = volt_rows[slot, c, pl.ds(begin, 16), :].astype(F32)
                            sums[u] = [sums[u][0] + wr * v, sums[u][1] + wi * v]
                for u in range(unroll):
                    begin = pl.multiple_of((s * unroll + u) * kept, 8)
                    for which in range(2):
                        value = sums[u][which]
                        value = value[:8] + value[8:]
                        rows = pl.ds(begin + (c * 2 + which) * 8, 8)
                        acc[slot, rows, :] = acc[slot, rows, :] + value if extend else value
            return carry

        lax.fori_loop(0, tb // unroll, step, 0)

    starts = [0]
    if exchange:
        starts = [pl.multiple_of(lax.rem(beam + db, nb) * share, 16) for db in range(nb)]
        weigh(starts[0], lambda c: gains[beam, c])
        for slot in range(nt):
            for load in loads[slot]:
                load.wait()
            accumulate(slot, starts[:1], False)
        for copy in gain_copies:
            copy.wait_recv()
        for db in range(1, nb):
            weigh(starts[db], lambda c, db=db: gains[lax.rem(beam + db, nb), c])
    else:
        weigh(0, lambda c: own_rows[c])
    part_copies = []
    for slot, d in enumerate(order):
        if exchange:
            accumulate(slot, starts[1:], True)
        else:
            for load in loads[slot]:
                load.wait()
            accumulate(slot, starts, False)

        def take(which, p, c, ri):
            total = None
            for half in range(2):
                start = (c * 2 + which) * 8 + half * 4 + p * 2 + ri
                value = acc[slot, pl.ds(start, tb, stride=kept), :]
                total = value if total is None else total + value
            return total

        for p in range(2):
            for c in range(cz):
                part[slot, p * 2 * cz + c] = take(0, p, c, 0) - take(1, p, c, 1)
                part[slot, (p * 2 + 1) * cz + c] = take(0, p, c, 1) + take(1, p, c, 0)
        if d:
            copy = pltpu.make_async_remote_copy(
                src_ref=part.at[slot],
                dst_ref=recv.at[slot],
                send_sem=part_send.at[slot],
                recv_sem=part_recv.at[slot],
                device_id=peer(lax.rem(tile + d, nt), chan, beam),
                device_id_type=MESH,
            )
            copy.start()
            part_copies.append(copy)

    for copy in part_copies:
        copy.wait_recv()

    def total_of(g, c):
        value = part[nt - 1, g * cz + c]
        for slot in range(nt - 1):
            value = value + recv[slot, g * cz + c]
        return value

    sums = jnp.concatenate(
        [jnp.concatenate([total_of(g, c) for c in range(cz)], axis=1) for g in range(4)], axis=0
    )
    high = sums.astype(BF16)
    low = (sums - high.astype(F32)).astype(BF16)
    for copy in small[4:]:
        copy.wait()
    table = perm_ref[...]
    moved = jnp.dot(high, table, preferred_element_type=F32) + jnp.dot(
        low, table, preferred_element_type=F32
    )
    group = lax.broadcasted_iota(jnp.int32, (tb, LANES), 1) // fz
    for z in range(nz):
        for c in range(cz):
            total = None
            for g in range(4):
                value = moved[g * tb : (g + 1) * tb, c * LANES : (c + 1) * LANES]
                shift = (g - z) * fz % LANES
                if shift:
                    value = pltpu.roll(value, shift, 1)
                total = value if g == 0 else jnp.where(group == g, value, total)
            packed[z, c] = total

    def pack_copy(h, dz):
        return pltpu.make_async_remote_copy(
            src_ref=packed.at[lax.rem(chan + dz, nz)],
            dst_ref=inbox.at[h, chan],
            send_sem=pack_send.at[h, dz],
            recv_sem=pack_recv.at[h, dz],
            device_id=peer(lax.rem(tile + h, nt), lax.rem(chan + dz, nz), beam),
            device_id_type=MESH,
        )

    spread = sorted(range(nz), key=lambda d: abs(2 * d - nz))
    for h in range(halo + 1):
        for dz in spread:
            if h == 0 and dz == 0:
                continue
            if h == 0:
                pack_copy(h, dz).start()
            else:

                @pl.when(tile + h < nt)
                def _():
                    pack_copy(h, dz).start()

    inbox[0, chan] = packed[chan]

    for copy in tables:
        copy.wait()
    for h in range(halo + 1):
        for dz in range(nz):
            if h == 0 and dz == 0:
                continue
            if h == 0:
                pack_copy(h, dz).wait_recv()
            else:

                @pl.when(tile >= h)
                def _():
                    pack_copy(h, dz).wait_recv()

    lhs = jnp.concatenate(
        [
            jnp.concatenate([inbox[h, z, c] for z in range(nz)], axis=1)
            for c in range(cz)
            for h in range(halo, -1, -1)
        ],
        axis=0,
    )
    high = lhs.astype(BF16)
    low = (lhs - high.astype(F32)).astype(BF16)
    spec[...] = (
        jnp.dot(high, dft_h[...], preferred_element_type=F32)
        + jnp.dot(low, dft_h[...], preferred_element_type=F32)
        + jnp.dot(high, dft_l[...], preferred_element_type=F32)
    )
    span = (halo + 1) * tb
    for c in range(cz):
        for g in range(4):
            total = None
            for k in range(taps):
                value = synth_ref[pl.ds(k, 1), :] * spec[
                    pl.ds(c * span + halo * tb - k, tb), g * LANES : (g + 1) * LANES
                ]
                total = value if total is None else total + value
            out_ref[c, :, g * LANES : (g + 1) * LANES] = total

    for copy in gain_copies:
        copy.wait_send()
    for copy in part_copies:
        copy.wait_send()
    for h in range(halo + 1):
        for dz in range(nz):
            if h == 0 and dz == 0:
                continue
            if h == 0:
                pack_copy(h, dz).wait_send()
            else:

                @pl.when(tile + h < nt)
                def _():
                    pack_copy(h, dz).wait_send()


def body(mesh, voltages, calib_gain, tile_flags, delays, pointing, synth_filter):
    nt, nz, nb = mesh.shape["tile"], mesh.shape["chan"], mesh.shape["beam"]
    total_rows, n_all = voltages.shape[:2]
    width = voltages.shape[-1]
    taps, k = synth_filter.shape
    tb = total_rows // nt
    fz = width // COARSE
    cz = COARSE // nz
    halo = -(-(taps - 1) // tb)
    n_own = calib_gain.shape[0]
    exchange = n_own % 4 == 0 and mesh.shape["beam"] > 1
    gain = calib_gain
    if not exchange:
        gain = gain * tile_flags.astype(F32)[:, None, None, None]
        gain = lax.all_gather(gain, "beam", axis=0, tiled=True)
    local = np.arange(width).reshape(-1, LANES)
    channel = (local % COARSE * k + local // COARSE).astype(np.float32)
    dft_h, dft_l = dft_table(nz, fz)
    perm = gather_table(nz, fz, cz)
    cfg = (nt, nz, nb, tb, n_all, taps, fz, cz, halo, exchange)
    vmem = pl.BlockSpec(memory_space=pltpu.VMEM)
    anywhere = pl.BlockSpec(memory_space=pl.ANY)
    span = (halo + 1) * tb
    dma = pltpu.SemaphoreType.DMA
    out = pl.pallas_call(
        functools.partial(kernel, cfg),
        out_shape=jax.ShapeDtypeStruct((cz, tb, 4 * k), F32),
        in_specs=[anywhere] * 10,
        out_specs=vmem,
        scratch_shapes=[
            pltpu.SMEM(tile_flags.shape, jnp.int32),
            pltpu.VMEM(delays.shape[::-1], F32),
            pltpu.SMEM(pointing.shape, jnp.int32),
            pltpu.VMEM(synth_filter.shape, F32),
            pltpu.VMEM(channel.shape, F32),
            pltpu.VMEM(perm.shape, BF16),
            dma((6,)),
            pltpu.VMEM((nt, cz, tb * n_all * 2, 2, LANES), BF16),
            pltpu.VMEM((cz, gain.shape[0] * 2, 2, LANES), F32),
            pltpu.VMEM((nb, cz, n_own * 4, LANES), F32),
            pltpu.VMEM((cz, n_all * 4, LANES), F32),
            pltpu.VMEM((cz, n_all * 4, LANES), F32),
            pltpu.VMEM((nt, tb * cz * 16, LANES), F32),
            pltpu.VMEM((nt, 4 * cz, tb, LANES), F32),
            pltpu.VMEM((nt - 1, 4 * cz, tb, LANES), F32),
            pltpu.VMEM((nz, cz, tb, LANES), F32),
            pltpu.VMEM((halo + 1, nz, cz, tb, LANES), F32),
            pltpu.VMEM((cz * span, 4 * k), F32),
            pltpu.VMEM(dft_h.shape, BF16),
            pltpu.VMEM(dft_l.shape, BF16),
            dma((nt, cz)),
            dma((2,)),
            dma((cz,)),
            dma((max(nb - 1, 1),)),
            dma((max(nb - 1, 1),)),
            dma((nt,)),
            dma((nt,)),
            dma((halo + 1, nz)),
            dma((halo + 1, nz)),
        ],
        compiler_params=pltpu.CompilerParams(collective_id=0, has_side_effects=True),
    )(
        voltages.reshape(-1, 2, width),
        gain.reshape(-1, 2, width),
        tile_flags,
        delays.T,
        pointing,
        synth_filter,
        jnp.asarray(channel),
        jnp.asarray(perm),
        jnp.asarray(dft_h),
        jnp.asarray(dft_l),
    )
    return out.reshape(cz, tb, 2, 2 * k).transpose(1, 2, 0, 3)[:, None]


def solution(mesh):
    in_specs = (
        P(None, "tile", None, None, "chan"),
        P(("tile", "beam"), None, None, "chan"),
        P(("tile", "beam")),
        P(None, "tile"),
        P("beam"),
        P(),
    )
    out_specs = P("tile", "beam", None, "chan", None)
    return jax.shard_map(
        functools.partial(body, mesh), mesh=mesh, in_specs=in_specs, out_specs=out_specs, check_vma=False
    )
```
